256 devices in a mesh: ga: 2 (over y), ea: 128 (over z, x, core).
Axes of the slice: x: 4, y: 2, z: 16, core: 2. Of those that a mesh axis runs over, the one named last changes fastest.
The devices are a block of a 4x16x16 slice.
Arguments:
- tokens: bfloat16 [32768, 2048], P(('ga', 'ea')), parts along dimension 0, may hold values from -6 to 6
- expert_choice_index: int32 [32768, 4], P(('ga', 'ea')), parts along dimension 0, may hold values from 0 to 63, all different within a row; in each aligned block of 128 rows (0 to 127, 128 to 255, ...) at most 9 rows name the same one
- router_gate_weight: float32 [32768, 4], P(('ga', 'ea')), parts along dimension 0, may hold values from 0.05 to 0.6
- cotangent: bfloat16 [32768, 2048], P(('ga', 'ea')), parts along dimension 0, may hold values from -6 to 6
- gate_up_matrix: bfloat16 [128, 2048, 1408], P('ea'), may hold values from -0.125 to 0.125
- down_weight: bfloat16 [128, 704, 2048], P('ea'), may hold values from -0.15625 to 0.15625
- adapter_input_projection: bfloat16 [2048, 16], replicated, may hold values from -0.125 to 0.125
- adapter_output_projection: bfloat16 [128, 16, 1408], P('ea'), may hold values from -0.59765625 to 0.59765625
Outputs:
- layer_output: bfloat16 [32768, 2048], P(('ga', 'ea')), parts along dimension 0
- adapter_input_gradient: float32 [4096, 16], P('ga'), parts along dimension 0
- lora_b_grad: float32 [256, 16, 1408], P(('ga', 'ea')), parts along dimension 0
The draws below stay inside these ranges and needn't reach their ends.
There are 2 independent parts, one for each index of `ga`. The reference program is written for one: setup_inputs(seed, part) draws one part's arguments, and reference() takes and returns one part's arrays. A program takes and returns all parts, laid end to end along the dimension named above; an argument that names none is the same for every part. Nothing has to cross between parts.
Inputs may be any that keep to these rules, and one draw needn't show every extreme that they name: `expert_choice_index`: each row names 4 different experts. Within the rows of one device (aligned blocks of 128 rows) no expert is named by more than 9 rows, and in every draw some expert is named by exactly 9 rows of some block.
All inputs are finite; a program needn't handle non-finite values.
Results may differ from the reference program's by a relative error of at most 0.0072.
Values may be sent and summed in bfloat16 or wider, within the bound.
No kernel may reach another device: no remote copies, remote signals or barrier semaphores. Data moves between devices by JAX's collectives and lax.ppermute only.
A program may use at most 128 MiB of HBM per device.

```python
import math
import jax
import jax.numpy as jnp
import numpy as np
from jax import lax

MODEL_DIM = 2048
FF = 1408
TOP = 4
ADAPTER_RANK = 16
EXPERT_SPLIT = 2
TOK_DEV = 128
EXPERT_COUNT = 64
BLOCK_HIDDEN = 704
HIDDEN_BLOCKS = 128
CAP = 9
TOKENS = 16384
N_EA = 128


def levels(rng, dims, split, smallest, top_value):
    level = 1.0
    for axis_at, shards_of in split:
        draws = jax.random.uniform(jax.random.fold_in(jax.random.fold_in(rng, 6), axis_at), (shards_of,), jnp.float32, smallest / len(split), top_value / len(split))
        level = level * jnp.repeat(jnp.exp(draws), dims[axis_at] // shards_of).reshape((-1,) + (1,) * (len(dims) - 1 - axis_at))
    return level


def assign_block(own_key, own, number, rows, number_of, top, reach, slope):
    sequence = jax.random.permutation(own_key, number_of)
    packed, usual = portions_of(number_of, rows * top, reach, slope, True), portions_of(number_of, rows * top, reach, slope, False)
    places = jnp.arange(number_of)

    def named(tallies, turn):
        used = int((tallies > 0).sum())
        fixed = max(1, used // 4)
        moved = fixed + (places - fixed + turn * (used - fixed)) % max(1, number_of - fixed)
        return jnp.zeros((number_of,), jnp.int32).at[sequence[jnp.where(places < fixed, places, moved)]].set(jnp.asarray(tallies, jnp.int32))

    tallies = jnp.where(number % 4 == 0, named(packed, number // 4), named(usual, number - number // 4 - 1))
    mixed = jax.random.permutation(jax.random.fold_in(own, 3), number_of)
    giver, receiver = mixed[0:number_of // 2 * 2:2], mixed[1:number_of // 2 * 2:2]
    margin = jnp.minimum(tallies[giver] - 1, reach - tallies[receiver]) // 2
    margin = jnp.where((giver == sequence[0]) | (receiver == sequence[0]) | (tallies[receiver] == 0), 0, jnp.maximum(margin, 0))
    moved = jax.random.randint(jax.random.fold_in(own, 4), (number_of // 2,), 0, 1 << 20) % (margin + 1)
    tallies = tallies.at[giver].add(-moved).at[receiver].add(moved)
    members = jnp.searchsorted(jnp.cumsum(tallies), jnp.arange(rows * top), side="right").astype(jnp.int32)
    listing = members.reshape(top, rows).T
    listing = listing[jax.random.permutation(jax.random.fold_in(own, 1), rows)]
    turn = jax.random.randint(jax.random.fold_in(own, 2), (rows, 1), 0, top)
    return jnp.take_along_axis(listing, (jnp.arange(top)[None, :] + turn) % top, axis=1)


def portions_of(amount, total, bound, skew, full):
    weights = [(1 << 20) // math.isqrt(rank ** skew) + 1 for rank in range(1, amount + 1)]
    largest = bound if full else min(bound, max(-(-total // amount), total * weights[0] // sum(weights)))
    least = 1 if total - largest >= amount - 1 else 0
    counts, surplus = [largest] + [least] * (amount - 1), total - largest - least * (amount - 1)
    while surplus > 0:
        free = [i for i in range(1, amount) if counts[i] < largest] or [i for i in range(1, amount) if counts[i] < bound]
        mass, left = sum([weights[i] for i in free]), surplus
        for i in free:
            addition = min(bound - counts[i], max(1, left * weights[i] // mass), surplus)
            counts[i] = counts[i] + addition
            surplus = surplus - addition
    return np.array(counts)


def normal_values(own_key, extent, width, most, pieces=(), kind=jnp.bfloat16):
    gain = levels(own_key, extent, pieces, -0.22, 0.18) if pieces else 1.0
    values = jax.random.normal(own_key, extent, jnp.float32) * width * gain
    return jnp.minimum(jnp.maximum(values, -most), most).astype(kind)


def setup_inputs(seed: int = 0, part: int = 0) -> dict:
    key_of = jax.random.split(jax.random.key(seed), 9)
    part_keys = jax.random.split(jax.random.fold_in(key_of[8], part), 9)
    tokens = normal_values(part_keys[0], (TOKENS, MODEL_DIM), 1.0, 6.0, ((0, 128),))
    expert_choice_index_keys = jax.random.split(jax.random.fold_in(part_keys[1], 1), TOKENS // TOK_DEV)
    expert_choice_index_turns = jax.random.permutation(jax.random.fold_in(part_keys[1], 3), TOKENS // TOK_DEV)
    expert_choice_index = jax.vmap(lambda own, number: assign_block(jax.random.fold_in(part_keys[1], 2), own, number, TOK_DEV, EXPERT_COUNT, TOP, CAP, 2))(expert_choice_index_keys, expert_choice_index_turns).reshape((TOKENS, TOP))
    router_gate_weight = jnp.clip(0.05 + 0.55 * jax.random.uniform(part_keys[2], (TOKENS, TOP), jnp.float32) ** levels(part_keys[2], (TOKENS, TOP), ((0, 128),), -0.2, 0.2), 0.05, 0.6)
    cotangent = normal_values(part_keys[3], (TOKENS, MODEL_DIM), 1.0, 6.0, ((0, 128),))
    gate_up_matrix = normal_values(key_of[4], (HIDDEN_BLOCKS, MODEL_DIM, 2 * BLOCK_HIDDEN), MODEL_DIM ** -0.5, 0.125, ((0, 128),))
    down_weight = normal_values(key_of[5], (HIDDEN_BLOCKS, BLOCK_HIDDEN, MODEL_DIM), FF ** -0.5, 0.15625, ((0, 128),))
    adapter_input_projection = normal_values(key_of[6], (MODEL_DIM, ADAPTER_RANK), MODEL_DIM ** -0.5, 0.125)
    adapter_output_projection = normal_values(key_of[7], (HIDDEN_BLOCKS, ADAPTER_RANK, 2 * BLOCK_HIDDEN), 0.1, 0.59765625, ((0, 128),))
    return {"tokens": tokens, "expert_choice_index": expert_choice_index, "router_gate_weight": router_gate_weight, "cotangent": cotangent, "gate_up_matrix": gate_up_matrix, "down_weight": down_weight, "adapter_input_projection": adapter_input_projection, "adapter_output_projection": adapter_output_projection}


adapter_scale = 2.0


def slot_ranks(id_block, experts):
    flat_ids = id_block.reshape(-1)
    onehot = (flat_ids[:, None] == jnp.arange(experts, dtype=jnp.int32)[None, :]).astype(jnp.int32)
    before = jnp.cumsum(onehot, axis=0) - onehot
    return jnp.sum(before * onehot, axis=1).reshape(id_block.shape).astype(jnp.int32)


def block_halfway(input_rows, output_gradient_rows, gate_up_weight, down_w, adapter_a, adapter_output_weight):
    adapter_input_rows = jnp.dot(input_rows, adapter_a, preferred_element_type=jnp.float32).astype(jnp.bfloat16)
    joined_columns = jnp.dot(input_rows, gate_up_weight, preferred_element_type=jnp.float32) + adapter_scale * jnp.dot(adapter_input_rows, adapter_output_weight, preferred_element_type=jnp.float32)
    block_width = down_w.shape[0]
    gate_part = joined_columns[:, :block_width]
    up_part = joined_columns[:, block_width:]
    sigmoid_gate = jax.nn.sigmoid(gate_part)
    active = gate_part * sigmoid_gate
    hidden = (active * up_part).astype(jnp.bfloat16)
    partial_value = jnp.dot(hidden, down_w, preferred_element_type=jnp.float32).astype(jnp.bfloat16)
    down_grad = lax.dot_general(output_gradient_rows, down_w, (((1,), (1,)), ((), ())), preferred_element_type=jnp.float32)
    gate_grad = down_grad * up_part * sigmoid_gate * (1.0 + gate_part * (1.0 - sigmoid_gate))
    up_grad = down_grad * active
    joined_gradient = jnp.concatenate([gate_grad, up_grad], axis=1).astype(jnp.bfloat16)
    output_gradient_part = adapter_scale * lax.dot_general(adapter_input_rows, joined_gradient, (((0,), (0,)), ((), ())), preferred_element_type=jnp.float32)
    adapter_gradient = (adapter_scale * lax.dot_general(joined_gradient, adapter_output_weight, (((1,), (1,)), ((), ())), preferred_element_type=jnp.float32)).astype(jnp.bfloat16)
    grad_a = lax.dot_general(input_rows, adapter_gradient, (((0,), (0,)), ((), ())), preferred_element_type=jnp.float32)
    return partial_value, grad_a, output_gradient_part


def reference(tokens, expert_choice_index, router_gate_weight, cotangent, gate_up_matrix, down_weight, adapter_input_projection, adapter_output_projection):
    def block_rank(id_block):
        return slot_ranks(id_block, EXPERT_COUNT)

    slot_rank = jax.vmap(block_rank)(expert_choice_index.reshape(N_EA, TOK_DEV, TOP)).reshape(TOKENS, TOP)
    source = (jnp.arange(TOKENS, dtype=jnp.int32) // TOK_DEV)[:, None] * jnp.ones((1, TOP), jnp.int32)
    token_index = jnp.arange(TOKENS, dtype=jnp.int32)[:, None] * jnp.ones((1, TOP), jnp.int32)
    slot_token = jnp.zeros((EXPERT_COUNT, N_EA, CAP), jnp.int32).at[expert_choice_index, source, slot_rank].set(token_index)
    slot_weight = jnp.zeros((EXPERT_COUNT, N_EA, CAP), jnp.float32).at[expert_choice_index, source, slot_rank].set(router_gate_weight)
    slot_filled = jnp.zeros((EXPERT_COUNT, N_EA, CAP), jnp.bool_).at[expert_choice_index, source, slot_rank].set(True)
    gate_up_pairs = gate_up_matrix.reshape(EXPERT_COUNT, EXPERT_SPLIT, MODEL_DIM, 2 * BLOCK_HIDDEN)
    down_pairs = down_weight.reshape(EXPERT_COUNT, EXPERT_SPLIT, BLOCK_HIDDEN, MODEL_DIM)
    adapter_couples = adapter_output_projection.reshape(EXPERT_COUNT, EXPERT_SPLIT, ADAPTER_RANK, 2 * BLOCK_HIDDEN)

    def one_expert(carry, inputs):
        out_sum, adapter_sum = carry
        index_rows, weight_rows, filled_rows, gate_up_couple, down_couple, adapter_couple = inputs
        slot_index = index_rows.reshape(-1).astype(jnp.int32)
        slot_prob = weight_rows.reshape(-1)
        filled_flag = filled_rows.reshape(-1)
        input_rows = jnp.where(filled_flag[:, None], tokens[slot_index], jnp.zeros((), jnp.bfloat16))
        output_gradient_rows = (slot_prob[:, None] * cotangent[slot_index].astype(jnp.float32)).astype(jnp.bfloat16)
        lower_block_part = block_halfway(input_rows, output_gradient_rows, gate_up_couple[0], down_couple[0], adapter_input_projection, adapter_couple[0])
        upper_block_part = block_halfway(input_rows, output_gradient_rows, gate_up_couple[1], down_couple[1], adapter_input_projection, adapter_couple[1])
        merged = (lower_block_part[0].astype(jnp.float32) + upper_block_part[0].astype(jnp.float32)).astype(jnp.bfloat16)
        out_sum = out_sum.at[slot_index].add(slot_prob[:, None] * merged.astype(jnp.float32))
        adapter_sum = adapter_sum + lower_block_part[1] + upper_block_part[1]
        return (out_sum, adapter_sum), jnp.stack([lower_block_part[2], upper_block_part[2]])

    start = (jnp.zeros((TOKENS, MODEL_DIM), jnp.float32), jnp.zeros((MODEL_DIM, ADAPTER_RANK), jnp.float32))
    (out_sum, adapter_sum), grads_b = lax.scan(one_expert, start, (slot_token, slot_weight, slot_filled, gate_up_pairs, down_pairs, adapter_couples))
    return out_sum.astype(jnp.bfloat16), adapter_sum, grads_b.reshape(HIDDEN_BLOCKS, ADAPTER_RANK, 2 * BLOCK_HIDDEN)
```

```python
import jax
import jax.numpy as jnp
import numpy as np
from jax import lax
from jax.sharding import Mesh
from jax.sharding import PartitionSpec as P

EXPERT_SPLIT = 2
EA = ("z", "x", "c")
GA_EA = ("ga", "z", "x", "c")
META = 128
X_FIRST = True


adapter_scale = 2.0
bf16 = jnp.bfloat16
f32 = jnp.float32


def up8(rows):
    return -(-rows // 8) * 8


def exact_parts(value):
    first = value.astype(bf16)
    rest = value - first.astype(f32)
    second = rest.astype(bf16)
    third = (rest - second.astype(f32)).astype(bf16)
    return first, second, third


def slot_ranks(ids, experts):
    rows = ids.shape[0]
    onehot = ids[:, :, None] == jnp.arange(experts, dtype=jnp.int32)[None, None, :]
    member = jnp.any(onehot, axis=1).astype(bf16)
    at = lax.broadcasted_iota(jnp.int32, (rows, rows), 0)
    earlier = lax.broadcasted_iota(jnp.int32, (rows, rows), 1)
    before = jnp.dot((earlier < at).astype(bf16), member, preferred_element_type=f32)
    return jnp.sum(jnp.where(onehot, before[:, None, :], 0.0), axis=2).astype(jnp.int32)


def farthest_first(far):
    rows = far.shape[0]
    this = lax.broadcasted_iota(jnp.int32, (rows, rows), 1)
    other = lax.broadcasted_iota(jnp.int32, (rows, rows), 0)
    ahead = (far[:, None] > far[None, :]) | ((far[:, None] == far[None, :]) & (other < this))
    place = jnp.sum(ahead.astype(jnp.int32), axis=0)
    return (other == place[None, :]).astype(bf16)


def pick(order, rows):
    return jnp.dot(order, rows, preferred_element_type=f32).astype(bf16)


def put_back(order, rows):
    return lax.dot_general(order, rows, (((0,), (0,)), ((), ())), preferred_element_type=f32)


def ring_pairs(planes, away):
    pairs = []
    for plane in range(planes):
        for core in range(2):
            step = away if core == 0 else -away
            pairs.append((plane * 2 + core, ((plane + step) % planes) * 2 + core))
    return pairs


def chips_along(value, distance):
    size = lax.axis_size("x")
    pairs = [(source, (source + distance) % size) for source in range(size)]
    return lax.ppermute(value, "x", pairs)


def swap_cores(value):
    return lax.ppermute(value, "c", [(0, 1), (1, 0)])


def rows_at(hop, hops, tok_rows, plane_rows):
    return min(tok_rows, up8(plane_rows * (hops + 1 - hop)))


def send_out(rows, pairs, hops, tok_rows, plane_rows):
    arrived = []
    for hop in range(1, hops + 1):
        rows = lax.ppermute(rows[: rows_at(hop, hops, tok_rows, plane_rows)], ("z", "c"), pairs)
        arrived.append(rows)
    return arrived


def bring_back(terms, pairs):
    total = terms[-1].astype(bf16)
    for hop in range(len(terms), 0, -1):
        total = lax.ppermute(total, ("z", "c"), pairs)
        if hop > 1:
            own = terms[hop - 2]
            more = own.shape[0] - total.shape[0]
            grown = jnp.pad(total, ((0, more), (0, 0))) if more else total
            total = (own + grown.astype(f32)).astype(bf16)
    return total


def selection(meta, place, capacity, span):
    planes, chips = lax.axis_size("z"), lax.axis_size("x")
    zi, xi = lax.axis_index("z"), lax.axis_index("x")
    top = 4
    slots = lax.broadcasted_iota(jnp.int32, (meta.shape[0], chips * span), 1)
    chosen = jnp.zeros(slots.shape, jnp.bool_)
    weight = jnp.zeros(slots.shape, f32)
    meta = meta.astype(f32)
    base = jnp.asarray(place * capacity)[:, None]
    for k in range(top):
        ids = meta[:, k : k + 1].astype(jnp.int32)
        rank = meta[:, top + k : top + k + 1].astype(jnp.int32)
        first = meta[:, 2 * top + k : 2 * top + k + 1]
        second = meta[:, 3 * top + k : 3 * top + k + 1]
        third = meta[:, 4 * top + k : 4 * top + k + 1]
        ahead = lax.rem(lax.rem(ids, chips) - xi + chips, chips)
        slot = jnp.where(ids // chips == zi, ahead * span + base + rank, -1)
        hit = slot == slots
        chosen = chosen | hit
        weight = weight + jnp.where(hit, first + second + third, 0.0)
    return chosen.astype(bf16), weight


def gather_rows(chosen, rows):
    return lax.dot_general(chosen, rows, (((0,), (0,)), ((), ())), preferred_element_type=f32)


def to_experts(rows):
    chips = lax.axis_size("x")
    span = rows.shape[0] // chips
    pieces = [rows[:span]]
    for distance in range(1, chips):
        pieces.append(chips_along(rows[distance * span : (distance + 1) * span], distance))
    own = jnp.concatenate(pieces, axis=0)
    return own, swap_cores(own)


def from_experts(rows):
    chips = lax.axis_size("x")
    span = rows.shape[0] // chips
    pieces = [rows[:span]]
    for distance in range(1, chips):
        pieces.append(chips_along(rows[distance * span : (distance + 1) * span], -distance))
    return jnp.concatenate(pieces, axis=0)


def halved(value, axis, bit, index):
    half = value.shape[axis] // 2
    low = lax.slice_in_dim(value, 0, half, axis=axis)
    high = lax.slice_in_dim(value, half, 2 * half, axis=axis)
    kept, given = jnp.where(bit == 0, low, high), jnp.where(bit == 0, high, low)
    return kept + index(given)


def doubled(value, axis, bit, index):
    other = index(value)
    return jnp.concatenate(
        [jnp.where(bit == 0, value, other), jnp.where(bit == 0, other, value)], axis=axis
    )


def flip(name, mask):
    def moved(value):
        size = lax.axis_size(name)
        return lax.ppermute(value, name, [(source, source ^ mask) for source in range(size)])

    return moved


def sum_over_group(value):
    ci, xi = lax.axis_index("c"), lax.axis_index("x")
    low, high = lax.rem(xi, 2), xi // 2
    value = halved(value, 0, ci, flip("c", 1))
    value = halved(value, 1, low, flip("x", 1))
    value = halved(value, 1, high, flip("x", 2))
    mask = 1
    while mask < lax.axis_size("z"):
        value = value + flip("z", mask)(value)
        mask *= 2
    value = doubled(value, 1, high, flip("x", 2))
    value = doubled(value, 1, low, flip("x", 1))
    return doubled(value, 0, ci, flip("c", 1))


def local(
    tokens,
    expert_choice_index,
    router_gate_weight,
    cotangent,
    gate_up_matrix,
    down_weight,
    adapter_input_projection,
    adapter_output_projection,
):
    planes, chips = lax.axis_size("z"), lax.axis_size("x")
    experts = planes * chips
    tok_rows, width = tokens.shape
    top = expert_choice_index.shape[1]
    capacity = 9 * tok_rows * top // (8 * experts)
    plane_rows = chips * capacity
    half = width // 2
    zi, ci = lax.axis_index("z"), lax.axis_index("c")
    hops_a, hops_b = planes // 2, planes // 2 - 1

    ids = expert_choice_index
    rank = slot_ranks(ids, experts)
    away = lax.rem((1 - 2 * ci) * (ids // chips - zi) + planes, planes)
    far_a = jnp.max(jnp.where(away <= hops_a, away, 0), axis=1)
    far_b = jnp.max(jnp.where(away > hops_a, planes - away, 0), axis=1)
    order_a, order_b = farthest_first(far_a), farthest_first(far_b)
    meta = jnp.concatenate(
        [ids.astype(bf16), rank.astype(bf16), *exact_parts(router_gate_weight)], axis=1
    )
    meta = jnp.pad(meta, ((0, 0), (0, META - meta.shape[1])))
    first_half = tokens[:, :half]
    second_half = jnp.concatenate([tokens[:, half:], meta], axis=1)

    out_a, out_b = ring_pairs(planes, 1), ring_pairs(planes, -1)
    sizes = (tok_rows, plane_rows)
    x1_a = send_out(pick(order_a, first_half), out_a, hops_a, *sizes)
    x1_b = send_out(pick(order_b, first_half), out_b, hops_b, *sizes)
    x2_a = send_out(pick(order_a, second_half), out_a, hops_a, *sizes)
    x2_b = send_out(pick(order_b, second_half), out_b, hops_b, *sizes)
    y_a, y_b = pick(order_a, cotangent), pick(order_b, cotangent)
    if X_FIRST:
        y_a, y_b, x2_a[-1], x2_b[-1], x1_a[-1], x1_b[-1] = lax.optimization_barrier(
            (y_a, y_b, x2_a[-1], x2_b[-1], x1_a[-1], x1_b[-1])
        )
    y_a = send_out(y_a, out_a, hops_a, *sizes)
    y_b = send_out(y_b, out_b, hops_b, *sizes)

    cut_a, cut_b = planes // 4, planes // 4 - 1
    span = (planes // 2) * capacity

    def grouped(own, from_a, from_b):
        near = [own] + from_a[:cut_a] + from_b[:cut_b]
        return near, from_a[cut_a:] + from_b[cut_b:]

    x_groups, y_groups, choices = [], [], []
    for ones, twos, ys in zip(
        grouped(first_half, x1_a, x1_b),
        grouped(second_half, x2_a, x2_b),
        grouped(cotangent, y_a, y_b),
    ):
        place = np.concatenate([np.full(rows.shape[0], at, np.int32) for at, rows in enumerate(ones)])
        ones = jnp.concatenate(ones, axis=0)
        twos = jnp.concatenate(twos, axis=0)
        chosen, weight = selection(twos[:, half:], place, capacity, span)
        picked = [gather_rows(chosen, ones).astype(bf16), gather_rows(chosen, twos[:, :half]).astype(bf16)]
        x_groups.extend(to_experts(jnp.concatenate(picked, axis=1)))
        slot_weight = jnp.sum(weight, axis=0)
        scaled = gather_rows(chosen, jnp.concatenate(ys, axis=0)) * slot_weight[:, None]
        y_groups.extend(to_experts(scaled.astype(bf16)))
        choices.append(weight)

    input_rows = jnp.concatenate(x_groups, axis=0)
    gate_up, down = gate_up_matrix[0], down_weight[0]
    adapter_out = adapter_output_projection[0]
    hidden_width = down.shape[0]
    adapter_in = jnp.dot(
        input_rows, adapter_input_projection, preferred_element_type=f32
    ).astype(bf16)
    joined = jnp.dot(input_rows, gate_up, preferred_element_type=f32) + adapter_scale * jnp.dot(
        adapter_in, adapter_out, preferred_element_type=f32
    )
    gate, up = joined[:, :hidden_width], joined[:, hidden_width:]
    sigmoid = jax.nn.sigmoid(gate)
    active = gate * sigmoid
    hidden = (active * up).astype(bf16)
    partial = jnp.dot(hidden, down, preferred_element_type=f32).astype(bf16)

    part = chips * span
    terms = []
    for at, weight in enumerate(choices):
        own = partial[2 * at * part : (2 * at + 1) * part]
        other = swap_cores(partial[(2 * at + 1) * part : (2 * at + 2) * part])
        summed = (own.astype(f32) + other.astype(f32)).astype(bf16)
        expert_out = from_experts(summed)
        high = weight.astype(bf16)
        low = (weight - high.astype(f32)).astype(bf16)
        terms.append(
            jnp.dot(high, expert_out, preferred_element_type=f32)
            + jnp.dot(low, expert_out, preferred_element_type=f32)
        )

    def cut_rows(value, counts):
        pieces, start = [], 0
        for count in counts:
            pieces.append(value[start : start + count])
            start += count
        return pieces

    count_a = [rows_at(hop, hops_a, *sizes) for hop in range(1, hops_a + 1)]
    count_b = [rows_at(hop, hops_b, *sizes) for hop in range(1, hops_b + 1)]
    near = cut_rows(terms[0], [tok_rows] + count_a[:cut_a] + count_b[:cut_b])
    far = cut_rows(terms[1], count_a[cut_a:] + count_b[cut_b:])
    term_a = near[1 : 1 + cut_a] + far[: hops_a - cut_a]
    term_b = near[1 + cut_a :] + far[hops_a - cut_a :]
    pieces = []
    for start in (0, half):
        cols = slice(start, start + half)
        home_a = bring_back([term[:, cols] for term in term_a], out_b)
        home_b = bring_back([term[:, cols] for term in term_b], out_a)
        total = near[0][:, cols] + put_back(order_a, home_a) + put_back(order_b, home_b)
        pieces.append(total.astype(bf16))
    layer_output = jnp.concatenate(pieces, axis=1)

    gradient_rows = jnp.concatenate(y_groups, axis=0)
    down_grad = lax.dot_general(
        gradient_rows, down, (((1,), (1,)), ((), ())), preferred_element_type=f32
    )
    gate_grad = down_grad * up * sigmoid * (1.0 + gate * (1.0 - sigmoid))
    up_grad = down_grad * active
    d_joined = jnp.concatenate([gate_grad, up_grad], axis=1).astype(bf16)
    lora_b_grad = adapter_scale * lax.dot_general(
        adapter_in, d_joined, (((0,), (0,)), ((), ())), preferred_element_type=f32
    )
    d_adapter = (
        adapter_scale
        * lax.dot_general(
            d_joined, adapter_out, (((1,), (1,)), ((), ())), preferred_element_type=f32
        )
    ).astype(bf16)
    grad_a = lax.dot_general(
        d_adapter, input_rows, (((0,), (0,)), ((), ())), preferred_element_type=f32
    )
    return layer_output, sum_over_group(grad_a).T, lora_b_grad[None]


def solution(mesh):
    split = Mesh(mesh.devices.reshape(mesh.shape["ga"], 16, 4, 2), GA_EA)
    in_specs = (
        P(GA_EA, None),
        P(GA_EA, None),
        P(GA_EA, None),
        P(GA_EA, None),
        P(EA, None, None),
        P(EA, None, None),
        P(),
        P(EA, None, None),
    )
    out_specs = (P(GA_EA, None), P("ga", None), P(GA_EA, None, None))
    return jax.shard_map(local, mesh=split, in_specs=in_specs, out_specs=out_specs, check_vma=False)
```

```python
import jax
import jax.numpy as jnp
import numpy as np
from jax import lax
from jax.sharding import Mesh
from jax.sharding import PartitionSpec as P

EXPERT_SPLIT = 2
EA = ("z", "x", "c")
GA_EA = ("ga", "z", "x", "c")
META = 128
TOP = 4
Y_AFTER = 4


adapter_scale = 2.0
bf16 = jnp.bfloat16
f32 = jnp.float32


def up8(rows):
    return -(-rows // 8) * 8


def exact_parts(value):
    first = value.astype(bf16)
    rest = value - first.astype(f32)
    second = rest.astype(bf16)
    third = (rest - second.astype(f32)).astype(bf16)
    return first, second, third


def slot_ranks(ids, experts):
    rows = ids.shape[0]
    onehot = ids[:, :, None] == jnp.arange(experts, dtype=jnp.int32)[None, None, :]
    member = jnp.any(onehot, axis=1).astype(bf16)
    at = lax.broadcasted_iota(jnp.int32, (rows, rows), 0)
    earlier = lax.broadcasted_iota(jnp.int32, (rows, rows), 1)
    before = jnp.dot((earlier < at).astype(bf16), member, preferred_element_type=f32)
    return jnp.sum(jnp.where(onehot, before[:, None, :], 0.0), axis=2).astype(jnp.int32)


def farthest_first(far):
    rows = far.shape[0]
    this = lax.broadcasted_iota(jnp.int32, (rows, rows), 1)
    other = lax.broadcasted_iota(jnp.int32, (rows, rows), 0)
    ahead = (far[:, None] > far[None, :]) | ((far[:, None] == far[None, :]) & (other < this))
    place = jnp.sum(ahead.astype(jnp.int32), axis=0)
    return (other == place[None, :]).astype(bf16)


def pick(order, rows):
    return jnp.dot(order, rows, preferred_element_type=f32).astype(bf16)


def ring_pairs(planes, away):
    pairs = []
    for plane in range(planes):
        for core in range(2):
            step = away if core == 0 else -away
            pairs.append((plane * 2 + core, ((plane + step) % planes) * 2 + core))
    return pairs


def chips_along(value, distance):
    size = lax.axis_size("x")
    pairs = [(source, (source + distance) % size) for source in range(size)]
    return lax.ppermute(value, "x", pairs)


def swap_cores(value):
    return lax.ppermute(value, "c", [(0, 1), (1, 0)])


def rows_at(hop, hops, tok_rows, plane_rows):
    return min(tok_rows, up8(plane_rows * (hops + 1 - hop)))


def send_out(rows, pairs, hops, tok_rows, plane_rows):
    arrived = []
    for hop in range(1, hops + 1):
        rows = lax.ppermute(rows[: rows_at(hop, hops, tok_rows, plane_rows)], ("z", "c"), pairs)
        arrived.append(rows)
    return arrived


def selection(meta, place, capacity, span):
    chips = lax.axis_size("x")
    zi, xi = lax.axis_index("z"), lax.axis_index("x")
    slots = lax.broadcasted_iota(jnp.int32, (meta.shape[0], chips * span), 1)
    chosen = jnp.zeros(slots.shape, jnp.bool_)
    meta = meta.astype(f32)
    base = jnp.asarray(place * capacity)[:, None]
    for k in range(TOP):
        ids = meta[:, k : k + 1].astype(jnp.int32)
        rank = meta[:, TOP + k : TOP + k + 1].astype(jnp.int32)
        ahead = lax.rem(lax.rem(ids, chips) - xi + chips, chips)
        slot = jnp.where(ids // chips == zi, ahead * span + base + rank, -1)
        chosen = chosen | (slot == slots)
    return chosen.astype(bf16)


def slot_table(meta, origin, tok_rows):
    chips = lax.axis_size("x")
    zi, xi = lax.axis_index("z"), lax.axis_index("x")
    span = meta.shape[0] // chips
    ahead = lax.broadcasted_iota(jnp.int32, (meta.shape[0], 1), 0) // span
    expert = zi * chips + lax.rem(xi + ahead, chips)
    filled = meta[:, 5 * TOP + 1 : 5 * TOP + 2] > 0.5
    weight = jnp.zeros((meta.shape[0], 1), f32)
    for k in range(TOP):
        value = (
            meta[:, 2 * TOP + k : 2 * TOP + k + 1]
            + meta[:, 3 * TOP + k : 3 * TOP + k + 1]
            + meta[:, 4 * TOP + k : 4 * TOP + k + 1]
        )
        hit = filled & (meta[:, k : k + 1].astype(jnp.int32) == expert)
        weight = weight + jnp.where(hit, value, 0.0)
    token = meta[:, 5 * TOP : 5 * TOP + 1].astype(jnp.int32)
    return jnp.where(filled, origin * tok_rows + token, -1), weight


def gather_rows(chosen, rows):
    return lax.dot_general(chosen, rows, (((0,), (0,)), ((), ())), preferred_element_type=f32)


def moved_over_chips(rows, way):
    chips = lax.axis_size("x")
    span = rows.shape[0] // chips
    pieces = [rows[:span]]
    for distance in range(1, chips):
        piece = rows[distance * span : (distance + 1) * span]
        pieces.append(chips_along(piece, way * distance))
    return pieces


def halved(value, axis, bit, index):
    half = value.shape[axis] // 2
    low = lax.slice_in_dim(value, 0, half, axis=axis)
    high = lax.slice_in_dim(value, half, 2 * half, axis=axis)
    kept, given = jnp.where(bit == 0, low, high), jnp.where(bit == 0, high, low)
    return kept + index(given)


def doubled(value, axis, bit, index):
    other = index(value)
    return jnp.concatenate(
        [jnp.where(bit == 0, value, other), jnp.where(bit == 0, other, value)], axis=axis
    )


def flip(name, mask):
    def moved(value):
        size = lax.axis_size(name)
        return lax.ppermute(value, name, [(source, source ^ mask) for source in range(size)])

    return moved


def sum_over_group(value):
    ci, xi = lax.axis_index("c"), lax.axis_index("x")
    low, high = lax.rem(xi, 2), xi // 2
    value = halved(value, 0, ci, flip("c", 1))
    value = halved(value, 1, low, flip("x", 1))
    value = halved(value, 1, high, flip("x", 2))
    mask = 1
    while mask < lax.axis_size("z"):
        value = value + flip("z", mask)(value)
        mask *= 2
    value = doubled(value, 1, high, flip("x", 2))
    value = doubled(value, 1, low, flip("x", 1))
    return doubled(value, 0, ci, flip("c", 1))


def local(
    tokens,
    expert_choice_index,
    router_gate_weight,
    cotangent,
    gate_up_matrix,
    down_weight,
    adapter_input_projection,
    adapter_output_projection,
):
    planes, chips = lax.axis_size("z"), lax.axis_size("x")
    experts = planes * chips
    tok_rows, width = tokens.shape
    capacity = 9 * tok_rows * TOP // (8 * experts)
    plane_rows = chips * capacity
    half = width // 2
    zi, ci = lax.axis_index("z"), lax.axis_index("c")
    hops_a, hops_b = planes // 2, planes // 2 - 1

    ids = expert_choice_index
    rank = slot_ranks(ids, experts)
    away = lax.rem((1 - 2 * ci) * (ids // chips - zi) + planes, planes)
    far_a = jnp.max(jnp.where(away <= hops_a, away, 0), axis=1)
    far_b = jnp.max(jnp.where(away > hops_a, planes - away, 0), axis=1)
    order_a, order_b = farthest_first(far_a), farthest_first(far_b)
    numbers = lax.broadcasted_iota(jnp.int32, (tok_rows, 1), 0).astype(bf16)
    meta = jnp.concatenate(
        [
            ids.astype(bf16),
            rank.astype(bf16),
            *exact_parts(router_gate_weight),
            numbers,
            jnp.ones_like(numbers),
        ],
        axis=1,
    )
    meta = jnp.pad(meta, ((0, 0), (0, META - meta.shape[1])))
    first_half = tokens[:, :half]
    second_half = jnp.concatenate([tokens[:, half:], meta], axis=1)

    out_a, out_b = ring_pairs(planes, 1), ring_pairs(planes, -1)
    sizes = (tok_rows, plane_rows)
    x1_a = send_out(pick(order_a, first_half), out_a, hops_a, *sizes)
    x1_b = send_out(pick(order_b, first_half), out_b, hops_b, *sizes)
    x2_a = send_out(pick(order_a, second_half), out_a, hops_a, *sizes)
    x2_b = send_out(pick(order_b, second_half), out_b, hops_b, *sizes)
    gated = lax.optimization_barrier((cotangent, x1_a[Y_AFTER], x1_b[Y_AFTER]))[0]
    all_cotangents = lax.all_gather(gated, "z", axis=0, tiled=True)

    cut_a, cut_b = planes // 4, planes // 4 - 1
    span = (planes // 2) * capacity

    def grouped(own, from_a, from_b):
        near = [own] + from_a[:cut_a] + from_b[:cut_b]
        return near, from_a[cut_a:] + from_b[cut_b:]

    steps = grouped([0], [[h] for h in range(1, hops_a + 1)], [[-h] for h in range(1, hops_b + 1)])
    steps = ([0] + [h[0] for h in steps[0][1:]], [h[0] for h in steps[1]])
    own_x, other_x, targets, weights = [], [], [], []
    for ones, twos, step in zip(
        grouped(first_half, x1_a, x1_b), grouped(second_half, x2_a, x2_b), steps
    ):
        place = np.concatenate([np.full(rows.shape[0], at, np.int32) for at, rows in enumerate(ones)])
        ones = jnp.concatenate(ones, axis=0)
        twos = jnp.concatenate(twos, axis=0)
        chosen = selection(twos[:, half:], place, capacity, span)
        got = gather_rows(chosen, twos)
        picked = [gather_rows(chosen, ones).astype(bf16), got[:, :half].astype(bf16)]
        own = moved_over_chips(jnp.concatenate(picked, axis=1), 1)
        other = swap_cores(jnp.concatenate(own, axis=0))
        own_x.append(own)
        other_x.append([other[at * span : (at + 1) * span] for at in range(chips)])
        step = jnp.asarray(np.tile(np.repeat(np.asarray(step, np.int32), capacity), chips))[:, None]
        origin = lax.rem(zi - (1 - 2 * ci) * step + 2 * planes, planes)
        target, weight = slot_table(got[:, half:], origin, tok_rows)
        targets.append([target[at * span : (at + 1) * span] for at in range(chips)])
        weights.append([weight[at * span : (at + 1) * span] for at in range(chips)])

    def in_order(groups):
        return [groups[group][at] for at in range(chips) for group in range(2)]

    target = jnp.concatenate(in_order(targets), axis=0)
    weight = jnp.concatenate(in_order(weights), axis=0)
    input_rows = jnp.concatenate(in_order(own_x) + in_order(other_x), axis=0)
    rows_here = input_rows.shape[0] // 2
    gate_up, down = gate_up_matrix[0], down_weight[0]
    adapter_out = adapter_output_projection[0]
    hidden_width = down.shape[0]
    adapter_in = jnp.dot(
        input_rows, adapter_input_projection, preferred_element_type=f32
    ).astype(bf16)
    joined = jnp.dot(input_rows, gate_up, preferred_element_type=f32) + adapter_scale * jnp.dot(
        adapter_in, adapter_out, preferred_element_type=f32
    )
    gate, up = joined[:, :hidden_width], joined[:, hidden_width:]
    sigmoid = jax.nn.sigmoid(gate)
    active = gate * sigmoid
    hidden = (active * up).astype(bf16)
    blocks = lax.broadcasted_iota(jnp.int32, (rows_here, planes * tok_rows), 1)
    places = target == blocks
    high = weight.astype(bf16).astype(f32)
    high_at = jnp.where(places, high, 0.0).astype(bf16)
    low_at = jnp.where(places, weight - high, 0.0).astype(bf16)
    outputs, partials = [], []
    for start in (0, half):
        partial = jnp.dot(hidden, down[:, start : start + half], preferred_element_type=f32).astype(bf16)
        partials.append(partial)
        other = swap_cores(partial[rows_here:])
        summed = (partial[:rows_here].astype(f32) + other.astype(f32)).astype(bf16)
        expert_out = jnp.concatenate(moved_over_chips(summed, -1), axis=0)
        sums = (gather_rows(high_at, expert_out) + gather_rows(low_at, expert_out)).astype(bf16)
        outputs.append(lax.psum_scatter(sums, "z", scatter_dimension=0, tiled=True))
    layer_output = jnp.concatenate(outputs, axis=1)

    all_cotangents = lax.optimization_barrier((all_cotangents, partials[1]))[0]
    scaled = jnp.dot(places.astype(bf16), all_cotangents, preferred_element_type=f32) * weight
    own_y = jnp.concatenate(moved_over_chips(scaled.astype(bf16), 1), axis=0)
    gradient_rows = jnp.concatenate([own_y, swap_cores(own_y)], axis=0)
    down_grad = lax.dot_general(
        gradient_rows, down, (((1,), (1,)), ((), ())), preferred_element_type=f32
    )
    gate_grad = down_grad * up * sigmoid * (1.0 + gate * (1.0 - sigmoid))
    up_grad = down_grad * active
    d_joined = jnp.concatenate([gate_grad, up_grad], axis=1).astype(bf16)
    lora_b_grad = adapter_scale * lax.dot_general(
        adapter_in, d_joined, (((0,), (0,)), ((), ())), preferred_element_type=f32
    )
    d_adapter = (
        adapter_scale
        * lax.dot_general(
            d_joined, adapter_out, (((1,), (1,)), ((), ())), preferred_element_type=f32
        )
    ).astype(bf16)
    grad_a = lax.dot_general(
        d_adapter, input_rows, (((0,), (0,)), ((), ())), preferred_element_type=f32
    )
    return layer_output, sum_over_group(grad_a).T, lora_b_grad[None]


def solution(mesh):
    split = Mesh(mesh.devices.reshape(mesh.shape["ga"], 16, 4, 2), GA_EA)
    in_specs = (
        P(GA_EA, None),
        P(GA_EA, None),
        P(GA_EA, None),
        P(GA_EA, None),
        P(EA, None, None),
        P(EA, None, None),
        P(),
        P(EA, None, None),
    )
    out_specs = (P(GA_EA, None), P("ga", None), P(GA_EA, None, None))
    return jax.shard_map(local, mesh=split, in_specs=in_specs, out_specs=out_specs, check_vma=False)
```

```python
import jax
import jax.numpy as jnp
import numpy as np
from jax import lax
from jax.sharding import Mesh
from jax.sharding import PartitionSpec as P

EXPERT_SPLIT = 2
EA = ("z", "x", "c")
GA_EA = ("ga", "z", "x", "c")
META = 128
TOP = 4
Y_AFTER = 5


adapter_scale = 2.0
bf16 = jnp.bfloat16
f32 = jnp.float32


def up8(rows):
    return -(-rows // 8) * 8


def exact_parts(value):
    first = value.astype(bf16)
    rest = value - first.astype(f32)
    second = rest.astype(bf16)
    third = (rest - second.astype(f32)).astype(bf16)
    return first, second, third


def slot_ranks(ids, experts):
    rows = ids.shape[0]
    onehot = ids[:, :, None] == jnp.arange(experts, dtype=jnp.int32)[None, None, :]
    member = jnp.any(onehot, axis=1).astype(bf16)
    at = lax.broadcasted_iota(jnp.int32, (rows, rows), 0)
    earlier = lax.broadcasted_iota(jnp.int32, (rows, rows), 1)
    before = jnp.dot((earlier < at).astype(bf16), member, preferred_element_type=f32)
    return jnp.sum(jnp.where(onehot, before[:, None, :], 0.0), axis=2).astype(jnp.int32)


def farthest_first(far):
    rows = far.shape[0]
    this = lax.broadcasted_iota(jnp.int32, (rows, rows), 1)
    other = lax.broadcasted_iota(jnp.int32, (rows, rows), 0)
    ahead = (far[:, None] > far[None, :]) | ((far[:, None] == far[None, :]) & (other < this))
    place = jnp.sum(ahead.astype(jnp.int32), axis=0)
    return (other == place[None, :]).astype(bf16)


def pick(order, rows):
    return jnp.dot(order, rows, preferred_element_type=f32).astype(bf16)


def ring_pairs(planes, away):
    pairs = []
    for plane in range(planes):
        for core in range(2):
            step = away if core == 0 else -away
            pairs.append((plane * 2 + core, ((plane + step) % planes) * 2 + core))
    return pairs


def chips_along(value, distance):
    size = lax.axis_size("x")
    pairs = [(source, (source + distance) % size) for source in range(size)]
    return lax.ppermute(value, "x", pairs)


def swap_cores(value):
    return lax.ppermute(value, "c", [(0, 1), (1, 0)])


def rows_at(hop, hops, tok_rows, plane_rows):
    return min(tok_rows, up8(plane_rows * (hops + 1 - hop)))


def send_out(rows, pairs, hops, tok_rows, plane_rows):
    arrived = []
    for hop in range(1, hops + 1):
        rows = lax.ppermute(rows[: rows_at(hop, hops, tok_rows, plane_rows)], ("z", "c"), pairs)
        arrived.append(rows)
    return arrived


def selection(meta, place, capacity, span):
    chips = lax.axis_size("x")
    zi, xi = lax.axis_index("z"), lax.axis_index("x")
    slots = lax.broadcasted_iota(jnp.int32, (meta.shape[0], chips * span), 1)
    chosen = jnp.zeros(slots.shape, jnp.bool_)
    meta = meta.astype(f32)
    base = jnp.asarray(place * capacity)[:, None]
    for k in range(TOP):
        ids = meta[:, k : k + 1].astype(jnp.int32)
        rank = meta[:, TOP + k : TOP + k + 1].astype(jnp.int32)
        ahead = lax.rem(lax.rem(ids, chips) - xi + chips, chips)
        slot = jnp.where(ids // chips == zi, ahead * span + base + rank, -1)
        chosen = chosen | (slot == slots)
    return chosen.astype(bf16)


def slot_table(meta, origin, tok_rows):
    chips = lax.axis_size("x")
    zi, xi = lax.axis_index("z"), lax.axis_index("x")
    span = meta.shape[0] // chips
    ahead = lax.broadcasted_iota(jnp.int32, (meta.shape[0], 1), 0) // span
    expert = zi * chips + lax.rem(xi + ahead, chips)
    lanes = lax.broadcasted_iota(jnp.int32, meta.shape, 1)

    def lane(number):
        return jnp.sum(jnp.where(lanes == number, meta, 0.0), axis=1, keepdims=True)

    filled = lane(5 * TOP + 1) > 0.5
    hit = filled & (lanes < TOP) & (meta == expert.astype(f32))
    source = lax.broadcasted_iota(jnp.int32, (META, META), 0)
    taken = lax.broadcasted_iota(jnp.int32, (META, META), 1)
    spread = (source < TOP) & (taken >= 2 * TOP) & (taken < 5 * TOP) & (taken % TOP == source)
    spread = jnp.dot(hit.astype(bf16), spread.astype(bf16), preferred_element_type=f32)
    weight = jnp.sum(spread * meta, axis=1, keepdims=True)
    token = lane(5 * TOP).astype(jnp.int32)
    return jnp.where(filled, origin * tok_rows + token, -1), weight


def gather_rows(chosen, rows):
    return lax.dot_general(chosen, rows, (((0,), (0,)), ((), ())), preferred_element_type=f32)


def moved_over_chips(rows, way):
    chips = lax.axis_size("x")
    span = rows.shape[0] // chips
    pieces = [rows[:span]]
    for distance in range(1, chips):
        piece = rows[distance * span : (distance + 1) * span]
        pieces.append(chips_along(piece, way * distance))
    return pieces


def halved(value, axis, bit, index):
    half = value.shape[axis] // 2
    low = lax.slice_in_dim(value, 0, half, axis=axis)
    high = lax.slice_in_dim(value, half, 2 * half, axis=axis)
    kept, given = jnp.where(bit == 0, low, high), jnp.where(bit == 0, high, low)
    return kept + index(given)


def doubled(value, axis, bit, index):
    other = index(value)
    return jnp.concatenate(
        [jnp.where(bit == 0, value, other), jnp.where(bit == 0, other, value)], axis=axis
    )


def flip(name, mask):
    def moved(value):
        size = lax.axis_size(name)
        return lax.ppermute(value, name, [(source, source ^ mask) for source in range(size)])

    return moved


def sum_over_group(value):
    ci, xi = lax.axis_index("c"), lax.axis_index("x")
    low, high = lax.rem(xi, 2), xi // 2
    value = halved(value, 0, ci, flip("c", 1))
    value = halved(value, 1, low, flip("x", 1))
    value = halved(value, 1, high, flip("x", 2))
    mask = 1
    while mask < lax.axis_size("z"):
        value = value + flip("z", mask)(value)
        mask *= 2
    value = doubled(value, 1, high, flip("x", 2))
    value = doubled(value, 1, low, flip("x", 1))
    return doubled(value, 0, ci, flip("c", 1))


def local(
    tokens,
    expert_choice_index,
    router_gate_weight,
    cotangent,
    gate_up_matrix,
    down_weight,
    adapter_input_projection,
    adapter_output_projection,
):
    planes, chips = lax.axis_size("z"), lax.axis_size("x")
    experts = planes * chips
    tok_rows, width = tokens.shape
    capacity = 9 * tok_rows * TOP // (8 * experts)
    plane_rows = chips * capacity
    half = width // 2
    zi, ci = lax.axis_index("z"), lax.axis_index("c")
    hops_a, hops_b = planes // 2, planes // 2 - 1

    ids = expert_choice_index
    rank = slot_ranks(ids, experts)
    away = lax.rem((1 - 2 * ci) * (ids // chips - zi) + planes, planes)
    far_a = jnp.max(jnp.where(away <= hops_a, away, 0), axis=1)
    far_b = jnp.max(jnp.where(away > hops_a, planes - away, 0), axis=1)
    order_a, order_b = farthest_first(far_a), farthest_first(far_b)
    numbers = lax.broadcasted_iota(jnp.int32, (tok_rows, 1), 0).astype(bf16)
    meta = jnp.concatenate(
        [
            ids.astype(bf16),
            rank.astype(bf16),
            *exact_parts(router_gate_weight),
            numbers,
            jnp.ones_like(numbers),
        ],
        axis=1,
    )
    meta = jnp.pad(meta, ((0, 0), (0, META - meta.shape[1])))
    first_half = tokens[:, :half]
    second_half = jnp.concatenate([tokens[:, half:], meta], axis=1)

    out_a, out_b = ring_pairs(planes, 1), ring_pairs(planes, -1)
    sizes = (tok_rows, plane_rows)
    x1_a = send_out(pick(order_a, first_half), out_a, hops_a, *sizes)
    x1_b = send_out(pick(order_b, first_half), out_b, hops_b, *sizes)
    x2_a = send_out(pick(order_a, second_half), out_a, hops_a, *sizes)
    x2_b = send_out(pick(order_b, second_half), out_b, hops_b, *sizes)
    gated = lax.optimization_barrier((cotangent, x1_a[Y_AFTER], x1_b[Y_AFTER]))[0]
    all_cotangents = lax.all_gather(gated, "z", axis=0, tiled=True)

    cut_a, cut_b = planes // 4, planes // 4 - 1
    span = (planes // 2) * capacity

    def grouped(own, from_a, from_b):
        near = [own] + from_a[:cut_a] + from_b[:cut_b]
        return near, from_a[cut_a:] + from_b[cut_b:]

    steps = grouped([0], [[h] for h in range(1, hops_a + 1)], [[-h] for h in range(1, hops_b + 1)])
    steps = ([0] + [h[0] for h in steps[0][1:]], [h[0] for h in steps[1]])
    own_x, other_x, targets, weights = [], [], [], []
    for ones, twos, step in zip(
        grouped(first_half, x1_a, x1_b), grouped(second_half, x2_a, x2_b), steps
    ):
        place = np.concatenate([np.full(rows.shape[0], at, np.int32) for at, rows in enumerate(ones)])
        ones = jnp.concatenate(ones, axis=0)
        twos = jnp.concatenate(twos, axis=0)
        chosen = selection(twos[:, half:], place, capacity, span)
        got = gather_rows(chosen, twos)
        picked = [gather_rows(chosen, ones).astype(bf16), got[:, :half].astype(bf16)]
        own = moved_over_chips(jnp.concatenate(picked, axis=1), 1)
        other = swap_cores(jnp.concatenate(own, axis=0))
        own_x.append(own)
        other_x.append([other[at * span : (at + 1) * span] for at in range(chips)])
        step = jnp.asarray(np.tile(np.repeat(np.asarray(step, np.int32), capacity), chips))[:, None]
        origin = lax.rem(zi - (1 - 2 * ci) * step + 2 * planes, planes)
        target, weight = slot_table(got[:, half:], origin, tok_rows)
        targets.append([target[at * span : (at + 1) * span] for at in range(chips)])
        weights.append([weight[at * span : (at + 1) * span] for at in range(chips)])

    def in_order(groups):
        return [groups[group][at] for at in range(chips) for group in range(2)]

    target = jnp.concatenate(in_order(targets), axis=0)
    weight = jnp.concatenate(in_order(weights), axis=0)
    input_rows = jnp.concatenate(in_order(own_x) + in_order(other_x), axis=0)
    rows_here = input_rows.shape[0] // 2
    blocks = lax.broadcasted_iota(jnp.int32, (rows_here, planes * tok_rows), 1)
    places = target == blocks
    places, weight, input_rows = lax.optimization_barrier(
        (places.astype(bf16), weight, input_rows)
    )
    gate_up, down = gate_up_matrix[0], down_weight[0]
    adapter_out = adapter_output_projection[0]
    hidden_width = down.shape[0]
    adapter_in = jnp.dot(
        input_rows, adapter_input_projection, preferred_element_type=f32
    ).astype(bf16)
    joined = jnp.dot(input_rows, gate_up, preferred_element_type=f32) + adapter_scale * jnp.dot(
        adapter_in, adapter_out, preferred_element_type=f32
    )
    gate, up = joined[:, :hidden_width], joined[:, hidden_width:]
    sigmoid = jax.nn.sigmoid(gate)
    active = gate * sigmoid
    hidden = (active * up).astype(bf16)
    arrived = []
    for start in (0, half):
        partial = jnp.dot(hidden, down[:, start : start + half], preferred_element_type=f32).astype(bf16)
        other = swap_cores(partial[rows_here:])
        summed = (partial[:rows_here].astype(f32) + other.astype(f32)).astype(bf16)
        arrived.append(jnp.concatenate(moved_over_chips(summed, -1), axis=0))
        last = partial
    all_cotangents = lax.optimization_barrier((all_cotangents, last))[0]
    scaled = jnp.dot(places, all_cotangents, preferred_element_type=f32) * weight
    weighted = (jnp.concatenate(arrived, axis=1).astype(f32) * weight).astype(bf16)
    scaled, weighted = lax.optimization_barrier((scaled.astype(bf16), weighted))
    sums = gather_rows(places, weighted)
    layer_output = lax.psum_scatter(sums.astype(bf16), "z", scatter_dimension=0, tiled=True)
    own_y = jnp.concatenate(moved_over_chips(scaled, 1), axis=0)
    gradient_rows = jnp.concatenate([own_y, swap_cores(own_y)], axis=0)
    down_grad = lax.dot_general(
        gradient_rows, down, (((1,), (1,)), ((), ())), preferred_element_type=f32
    )
    gate_grad = down_grad * up * sigmoid * (1.0 + gate * (1.0 - sigmoid))
    up_grad = down_grad * active
    d_joined = jnp.concatenate([gate_grad, up_grad], axis=1).astype(bf16)
    lora_b_grad = adapter_scale * lax.dot_general(
        adapter_in, d_joined, (((0,), (0,)), ((), ())), preferred_element_type=f32
    )
    d_adapter = (
        adapter_scale
        * lax.dot_general(
            d_joined, adapter_out, (((1,), (1,)), ((), ())), preferred_element_type=f32
        )
    ).astype(bf16)
    grad_a = lax.dot_general(
        d_adapter, input_rows, (((0,), (0,)), ((), ())), preferred_element_type=f32
    )
    return layer_output, sum_over_group(grad_a).T, lora_b_grad[None]


def solution(mesh):
    split = Mesh(mesh.devices.reshape(mesh.shape["ga"], 16, 4, 2), GA_EA)
    in_specs = (
        P(GA_EA, None),
        P(GA_EA, None),
        P(GA_EA, None),
        P(GA_EA, None),
        P(EA, None, None),
        P(EA, None, None),
        P(),
        P(EA, None, None),
    )
    out_specs = (P(GA_EA, None), P("ga", None), P(GA_EA, None, None))
    return jax.shard_map(local, mesh=split, in_specs=in_specs, out_specs=out_specs, check_vma=False)
```

```python
import jax
import jax.numpy as jnp
import numpy as np
from jax import lax
from jax.sharding import Mesh
from jax.sharding import PartitionSpec as P


EA = ("z", "x", "c")
GA_EA = ("ga", "z", "x", "c")
META = 128
TOP = 4
Y_AFTER = 4


adapter_scale = 2.0
bf16 = jnp.bfloat16
f32 = jnp.float32


def up8(rows):
    return -(-rows // 8) * 8


def exact_parts(value):
    first = value.astype(bf16)
    rest = value - first.astype(f32)
    second = rest.astype(bf16)
    third = (rest - second.astype(f32)).astype(bf16)
    return first, second, third


def slot_ranks(ids, experts):
    rows = ids.shape[0]
    onehot = ids[:, :, None] == jnp.arange(experts, dtype=jnp.int32)[None, None, :]
    member = jnp.any(onehot, axis=1).astype(bf16)
    at = lax.broadcasted_iota(jnp.int32, (rows, rows), 0)
    earlier = lax.broadcasted_iota(jnp.int32, (rows, rows), 1)
    before = jnp.dot((earlier < at).astype(bf16), member, preferred_element_type=f32)
    return jnp.sum(jnp.where(onehot, before[:, None, :], 0.0), axis=2).astype(jnp.int32)


def farthest_first(far):
    rows = far.shape[0]
    this = lax.broadcasted_iota(jnp.int32, (rows, rows), 1)
    other = lax.broadcasted_iota(jnp.int32, (rows, rows), 0)
    ahead = (far[:, None] > far[None, :]) | ((far[:, None] == far[None, :]) & (other < this))
    place = jnp.sum(ahead.astype(jnp.int32), axis=0)
    return (other == place[None, :]).astype(bf16)


def pick(order, rows):
    return jnp.dot(order, rows, preferred_element_type=f32).astype(bf16)


def ring_pairs(planes, away):
    pairs = []
    for plane in range(planes):
        for core in range(2):
            step = away if core == 0 else -away
            pairs.append((plane * 2 + core, ((plane + step) % planes) * 2 + core))
    return pairs


def chips_along(value, distance):
    size = lax.axis_size("x")
    pairs = [(source, (source + distance) % size) for source in range(size)]
    return lax.ppermute(value, "x", pairs)


def swap_cores(value):
    return lax.ppermute(value, "c", [(0, 1), (1, 0)])


def rows_at(hop, hops, tok_rows, plane_rows):
    return min(tok_rows, up8(plane_rows * (hops + 1 - hop)))


def send_out(rows, pairs, hops, tok_rows, plane_rows):
    arrived = []
    for hop in range(1, hops + 1):
        rows = lax.ppermute(rows[: rows_at(hop, hops, tok_rows, plane_rows)], ("z", "c"), pairs)
        arrived.append(rows)
    return arrived


def selection(meta, place, capacity, span):
    chips = lax.axis_size("x")
    zi, xi = lax.axis_index("z"), lax.axis_index("x")
    slots = lax.broadcasted_iota(jnp.int32, (meta.shape[0], chips * span), 1)
    chosen = jnp.zeros(slots.shape, jnp.bool_)
    meta = meta.astype(f32)
    base = jnp.asarray(place * capacity)[:, None]
    for k in range(TOP):
        ids = meta[:, k : k + 1].astype(jnp.int32)
        rank = meta[:, TOP + k : TOP + k + 1].astype(jnp.int32)
        ahead = lax.rem(lax.rem(ids, chips) - xi + chips, chips)
        slot = jnp.where(ids // chips == zi, ahead * span + base + rank, -1)
        chosen = chosen | (slot == slots)
    return chosen.astype(bf16)


def slot_table(meta, origin, tok_rows):
    chips = lax.axis_size("x")
    zi, xi = lax.axis_index("z"), lax.axis_index("x")
    span = meta.shape[0] // chips
    ahead = lax.broadcasted_iota(jnp.int32, (meta.shape[0], 1), 0) // span
    expert = zi * chips + lax.rem(xi + ahead, chips)
    lanes = lax.broadcasted_iota(jnp.int32, meta.shape, 1)

    def lane(number):
        return jnp.sum(jnp.where(lanes == number, meta, 0.0), axis=1, keepdims=True)

    filled = lane(5 * TOP + 1) > 0.5
    hit = filled & (lanes < TOP) & (meta == expert.astype(f32))
    source = lax.broadcasted_iota(jnp.int32, (META, META), 0)
    taken = lax.broadcasted_iota(jnp.int32, (META, META), 1)
    spread = (source < TOP) & (taken >= 2 * TOP) & (taken < 5 * TOP) & (taken % TOP == source)
    spread = jnp.dot(hit.astype(bf16), spread.astype(bf16), preferred_element_type=f32)
    weight = jnp.sum(spread * meta, axis=1, keepdims=True)
    token = lane(5 * TOP).astype(jnp.int32)
    return jnp.where(filled, origin * tok_rows + token, -1), weight


def gather_rows(chosen, rows):
    return lax.dot_general(chosen, rows, (((0,), (0,)), ((), ())), preferred_element_type=f32)


def moved_over_chips(rows, way):
    chips = lax.axis_size("x")
    span = rows.shape[0] // chips
    pieces = [rows[:span]]
    for distance in range(1, chips):
        piece = rows[distance * span : (distance + 1) * span]
        pieces.append(chips_along(piece, way * distance))
    return pieces


def halved(value, axis, bit, index):
    half = value.shape[axis] // 2
    low = lax.slice_in_dim(value, 0, half, axis=axis)
    high = lax.slice_in_dim(value, half, 2 * half, axis=axis)
    kept, given = jnp.where(bit == 0, low, high), jnp.where(bit == 0, high, low)
    return kept + index(given)


def doubled(value, axis, bit, index):
    other = index(value)
    return jnp.concatenate(
        [jnp.where(bit == 0, value, other), jnp.where(bit == 0, other, value)], axis=axis
    )


def flip(name, mask):
    def moved(value):
        size = lax.axis_size(name)
        return lax.ppermute(value, name, [(source, source ^ mask) for source in range(size)])

    return moved


def sum_over_group(value):
    ci, xi = lax.axis_index("c"), lax.axis_index("x")
    low, high = lax.rem(xi, 2), xi // 2
    value = halved(value, 0, ci, flip("c", 1))
    value = halved(value, 1, low, flip("x", 1))
    value = halved(value, 1, high, flip("x", 2))
    mask = 1
    while mask < lax.axis_size("z"):
        value = value + flip("z", mask)(value)
        mask *= 2
    value = doubled(value, 1, high, flip("x", 2))
    value = doubled(value, 1, low, flip("x", 1))
    return doubled(value, 0, ci, flip("c", 1))


def local(
    tokens,
    expert_choice_index,
    router_gate_weight,
    cotangent,
    gate_up_matrix,
    down_weight,
    adapter_input_projection,
    adapter_output_projection,
):
    planes, chips = lax.axis_size("z"), lax.axis_size("x")
    experts = planes * chips
    tok_rows, width = tokens.shape
    capacity = 9 * tok_rows * TOP // (8 * experts)
    plane_rows = chips * capacity
    half = width // 2
    zi, ci = lax.axis_index("z"), lax.axis_index("c")
    hops_a, hops_b = planes // 2, planes // 2 - 1

    ids = expert_choice_index
    rank = slot_ranks(ids, experts)
    away = lax.rem((1 - 2 * ci) * (ids // chips - zi) + planes, planes)
    far_a = jnp.max(jnp.where(away <= hops_a, away, 0), axis=1)
    far_b = jnp.max(jnp.where(away > hops_a, planes - away, 0), axis=1)
    order_a, order_b = farthest_first(far_a), farthest_first(far_b)
    numbers = lax.broadcasted_iota(jnp.int32, (tok_rows, 1), 0).astype(bf16)
    meta = jnp.concatenate(
        [
            ids.astype(bf16),
            rank.astype(bf16),
            *exact_parts(router_gate_weight),
            numbers,
            jnp.ones_like(numbers),
        ],
        axis=1,
    )
    meta = jnp.pad(meta, ((0, 0), (0, META - meta.shape[1])))
    first_half = tokens[:, :half]
    second_half = jnp.concatenate([tokens[:, half:], meta], axis=1)

    out_a, out_b = ring_pairs(planes, 1), ring_pairs(planes, -1)
    sizes = (tok_rows, plane_rows)
    x1_a = send_out(pick(order_a, first_half), out_a, hops_a, *sizes)
    x1_b = send_out(pick(order_b, first_half), out_b, hops_b, *sizes)
    x2_a = send_out(pick(order_a, second_half), out_a, hops_a, *sizes)
    x2_b = send_out(pick(order_b, second_half), out_b, hops_b, *sizes)
    gated = lax.optimization_barrier((cotangent, x1_a[Y_AFTER], x1_b[Y_AFTER]))[0]
    all_cotangents = lax.all_gather(gated, "z", axis=0, tiled=True)

    cut_a, cut_b = planes // 4, planes // 4 - 1
    span = (planes // 2) * capacity

    def grouped(own, from_a, from_b):
        near = [own] + from_a[:cut_a] + from_b[:cut_b]
        return near, from_a[cut_a:] + from_b[cut_b:]

    steps = grouped([0], [[h] for h in range(1, hops_a + 1)], [[-h] for h in range(1, hops_b + 1)])
    steps = ([0] + [h[0] for h in steps[0][1:]], [h[0] for h in steps[1]])
    own_x, other_x, targets, weights = [], [], [], []
    for ones, twos, step in zip(
        grouped(first_half, x1_a, x1_b), grouped(second_half, x2_a, x2_b), steps
    ):
        place = np.concatenate([np.full(rows.shape[0], at, np.int32) for at, rows in enumerate(ones)])
        ones = jnp.concatenate(ones, axis=0)
        twos = jnp.concatenate(twos, axis=0)
        chosen = selection(twos[:, half:], place, capacity, span)
        got = gather_rows(chosen, twos)
        picked = [gather_rows(chosen, ones).astype(bf16), got[:, :half].astype(bf16)]
        own = moved_over_chips(jnp.concatenate(picked, axis=1), 1)
        own = lax.optimization_barrier(jnp.concatenate(own, axis=0))
        own_x.append(own)
        other_x.append(swap_cores(own))
        step = jnp.asarray(np.tile(np.repeat(np.asarray(step, np.int32), capacity), chips))[:, None]
        origin = lax.rem(zi - (1 - 2 * ci) * step + 2 * planes, planes)
        target, weight = slot_table(got[:, half:], origin, tok_rows)
        targets.append([target[at * span : (at + 1) * span] for at in range(chips)])
        weights.append([weight[at * span : (at + 1) * span] for at in range(chips)])

    def in_order(groups):
        return [groups[group][at] for at in range(chips) for group in range(2)]

    target = jnp.concatenate(in_order(targets), axis=0)
    weight = jnp.concatenate(in_order(weights), axis=0)
    input_rows = jnp.concatenate(own_x + other_x, axis=0)
    rows_here = input_rows.shape[0] // 2
    blocks = lax.broadcasted_iota(jnp.int32, (rows_here, planes * tok_rows), 1)
    places = (target == blocks).astype(bf16)
    blocks = lax.broadcasted_iota(jnp.int32, (planes * tok_rows, rows_here), 0)
    places_back = (target.reshape(1, rows_here) == blocks).astype(bf16)
    places, places_back, weight = lax.optimization_barrier((places, places_back, weight))
    gate_up, down = gate_up_matrix[0], down_weight[0]
    adapter_out = adapter_output_projection[0]
    hidden_width = down.shape[0]
    adapter_in = jnp.dot(
        input_rows, adapter_input_projection, preferred_element_type=f32
    ).astype(bf16)
    joined = jnp.dot(input_rows, gate_up, preferred_element_type=f32) + adapter_scale * jnp.dot(
        adapter_in, adapter_out, preferred_element_type=f32
    )
    gate, up = joined[:, :hidden_width], joined[:, hidden_width:]
    sigmoid = jax.nn.sigmoid(gate)
    active = gate * sigmoid
    hidden = (active * up).astype(bf16)
    arrived = []
    for start in (0, half):
        partial = jnp.dot(hidden, down[:, start : start + half], preferred_element_type=f32).astype(bf16)
        other = swap_cores(partial[rows_here:])
        summed = (partial[:rows_here].astype(f32) + other.astype(f32)).astype(bf16)
        near, far = summed[: rows_here // 2], summed[rows_here // 2 :]
        pieces = [rows[at * span : (at + 1) * span] for at in range(chips) for rows in (near, far)]
        arrived.append(
            jnp.concatenate(moved_over_chips(jnp.concatenate(pieces, axis=0), -1), axis=0)
        )
        last = partial
    all_cotangents = lax.optimization_barrier((all_cotangents, last))[0]
    scaled = jnp.dot(places, all_cotangents, preferred_element_type=f32) * weight
    weighted = (jnp.concatenate(arrived, axis=1).astype(f32) * weight).astype(bf16)
    sums = jnp.dot(places_back, weighted, preferred_element_type=f32)
    layer_output = lax.psum_scatter(sums.astype(bf16), "z", scatter_dimension=0, tiled=True)
    pieces = moved_over_chips(scaled.astype(bf16), 1)
    pieces = [piece[:span] for piece in pieces] + [piece[span:] for piece in pieces]
    own_y = jnp.concatenate(pieces, axis=0)
    gradient_rows = jnp.concatenate([own_y, swap_cores(own_y)], axis=0)
    down_grad = lax.dot_general(
        gradient_rows, down, (((1,), (1,)), ((), ())), preferred_element_type=f32
    )
    gate_grad = down_grad * up * sigmoid * (1.0 + gate * (1.0 - sigmoid))
    up_grad = down_grad * active
    d_joined = jnp.concatenate([gate_grad, up_grad], axis=1).astype(bf16)
    lora_b_grad = adapter_scale * lax.dot_general(
        adapter_in, d_joined, (((0,), (0,)), ((), ())), preferred_element_type=f32
    )
    d_adapter = (
        adapter_scale
        * lax.dot_general(
            d_joined, adapter_out, (((1,), (1,)), ((), ())), preferred_element_type=f32
        )
    ).astype(bf16)
    grad_a = lax.dot_general(
        d_adapter, input_rows, (((0,), (0,)), ((), ())), preferred_element_type=f32
    )
    return layer_output, sum_over_group(grad_a).T, lora_b_grad[None]


def solution(mesh):
    split = Mesh(mesh.devices.reshape(mesh.shape["ga"], 16, 4, 2), GA_EA)
    in_specs = (
        P(GA_EA, None),
        P(GA_EA, None),
        P(GA_EA, None),
        P(GA_EA, None),
        P(EA, None, None),
        P(EA, None, None),
        P(),
        P(EA, None, None),
    )
    out_specs = (P(GA_EA, None), P("ga", None), P(GA_EA, None, None))

    return jax.shard_map(local, mesh=split, in_specs=in_specs, out_specs=out_specs, check_vma=False)
```
